256 devices in a mesh: shuffle: 64 (over y, z, core), dp: 4 (over x).
Axes of the slice: x: 4, y: 4, z: 8, core: 2. Of those that a mesh axis runs over, the one named last changes fastest.
Arguments:
- fact_rows: bfloat16 [1048576, 512], P(('shuffle', 'dp')), may hold values from -6 to 6
- owner_index: int32 [1048576, 1], P(('shuffle', 'dp')), may hold values from 0 to 63, as said below
- light_slot: int32 [1048576, 1], P(('shuffle', 'dp')), may hold values from 0 to 1023
- heavy_flag: int32 [1048576, 1], P(('shuffle', 'dp')), may hold values from 0 to 1
- heavy_key: int32 [1048576, 1], P(('shuffle', 'dp')), may hold values from 0 to 1023
- light_dims: bfloat16 [65536, 512], P('shuffle', 'dp'), may hold values from -4 to 4
- heavy_dims: bfloat16 [1024, 512], P(('shuffle', 'dp')), may hold values from -1.5 to 1.5
Outputs:
- light_joined: bfloat16 [65536, 512], P('shuffle', 'dp')
- heavy_joined: bfloat16 [1024, 512], replicated
The draws below stay inside these ranges and needn't reach their ends.
Inputs may be any that keep to these rules, and one draw needn't show every extreme that they name: `owner_index`: among the rows of one device at most 96 name the same owner, and in every draw some device has exactly 96 rows with heavy_flag 0 that name one owner.
All inputs are finite; a program needn't handle non-finite values.
Results may differ from the reference program's by a relative error of at most 0.001.
Values may be sent and summed in bfloat16 or wider, within the bound.
A program may use at most 64 MiB of HBM per device.

```python
import jax
import jax.numpy as jnp
from jax import lax

F = 512
H = 1024
SLOTS = 1024
ROWS_DEV = 4096
CAP = 96
ROWS = 1048576
N_SHUFFLE = 64
DEVICES = 256


def owners_and_flags(key):
    base = jax.random.fold_in(key, 7123)
    keys = jax.random.split(base, 7)
    slot_count = N_SHUFFLE * CAP
    slot_owner = jnp.arange(slot_count, dtype=jnp.int32) // CAP
    owner_bias = jax.random.randint(keys[0], (N_SHUFFLE,), 0, 32768, dtype=jnp.int32)
    noise = jax.random.randint(keys[1], (DEVICES, slot_count), 0, 32768, dtype=jnp.int32)
    crowded = jax.random.randint(keys[2], (DEVICES,), 0, N_SHUFFLE, dtype=jnp.int32)
    picked_device = jax.random.randint(keys[3], (), 0, DEVICES, dtype=jnp.int32)
    device_ids = jnp.arange(DEVICES, dtype=jnp.int32)
    forced_device = (jax.random.randint(keys[4], (DEVICES,), 0, 8, dtype=jnp.int32) == 0) | (device_ids == picked_device)
    forced_slot = forced_device[:, None] & (slot_owner[None, :] == crowded[:, None])
    score = noise + owner_bias[slot_owner][None, :] + jnp.where(forced_slot, 65536, 0).astype(jnp.int32)
    distinct = score * slot_count + jnp.arange(slot_count, dtype=jnp.int32)[None, :]
    _, chosen = lax.top_k(distinct, ROWS_DEV)
    row_keys = jax.random.split(keys[5], DEVICES)
    chosen = jax.vmap(lambda part_key, picked: jax.random.permutation(part_key, picked))(row_keys, chosen.astype(jnp.int32))
    owners = (chosen // CAP).astype(jnp.int32)
    heavy = jax.random.randint(keys[6], (DEVICES, ROWS_DEV), 0, 4, dtype=jnp.int32) == 0
    forced_row = forced_device[:, None] & (owners == crowded[:, None])
    flags = jnp.where(heavy & jnp.logical_not(forced_row), 1, 0).astype(jnp.int32)
    return (owners.reshape(ROWS, 1), flags.reshape(ROWS, 1))


def draw_owner_index(key, part):
    return owners_and_flags(key)[0]


def draw_heavy_flag(key, part):
    return owners_and_flags(key)[1]


def with_ends(drawn, stream_key, low, top_value):
    extent = drawn.shape
    spot = [jax.random.randint(jax.random.fold_in(stream_key, axis), (), 0, extent[axis]) for axis in range(len(extent))]
    drawn = drawn.at[tuple(spot)].set(low)
    longest = extent.index(max(extent))
    spot[longest] = (spot[longest] + 1) % extent[longest]
    return drawn.at[tuple(spot)].set(top_value)


def block_scale(rng, dims, pieces, least, largest):
    loudness = 1.0
    for axis_at, parts in pieces:
        heights = jax.random.uniform(jax.random.fold_in(jax.random.fold_in(rng, 6), axis_at), (parts,), jnp.float32, least / len(pieces), largest / len(pieces))
        loudness = loudness * jnp.repeat(jnp.exp(heights), dims[axis_at] // parts).reshape((-1,) + (1,) * (len(dims) - 1 - axis_at))
    return loudness


def scatter_about(key, shape, scale, reach, cuts=(), held_as=jnp.bfloat16):
    gain = block_scale(key, shape, cuts, -0.22, 0.18) if cuts else 1.0
    result = jax.random.normal(key, shape, jnp.float32) * scale * gain
    return jnp.minimum(jnp.maximum(result, -reach), reach).astype(held_as)


def setup_inputs(seed: int = 0) -> dict:
    key_of = jax.random.split(jax.random.key(seed), 8)
    return {
        "fact_rows": scatter_about(key_of[0], (ROWS, F), 1.0, 6.0, ((0, 256),)),
        "owner_index": draw_owner_index(jax.random.fold_in(key_of[7], 71), 0),
        "light_slot": with_ends(jax.random.randint(key_of[2], (ROWS, 1), 0, SLOTS), jax.random.fold_in(key_of[2], 1), 0, SLOTS - 1).astype(jnp.int32),
        "heavy_flag": draw_heavy_flag(jax.random.fold_in(key_of[7], 71), 0),
        "heavy_key": with_ends(jax.random.randint(key_of[4], (ROWS, 1), 0, H), jax.random.fold_in(key_of[4], 1), 0, H - 1).astype(jnp.int32),
        "light_dims": scatter_about(key_of[5], (N_SHUFFLE * SLOTS, F), 0.3, 4.0, ((0, 64), (1, 4))),
        "heavy_dims": scatter_about(key_of[6], (H, F), 0.1, 1.5, ((0, 256),)),
    }


def reference(fact_rows, owner_index, light_slot, heavy_flag, heavy_key, light_dims, heavy_dims):
    light_count = N_SHUFFLE * SLOTS
    row_key = (owner_index[:, 0] * SLOTS + light_slot[:, 0]).astype(jnp.int32)
    light_key = jnp.where(heavy_flag[:, 0] == 0, row_key, light_count).astype(jnp.int32)
    heavy_index = jnp.where(heavy_flag[:, 0] == 1, heavy_key[:, 0], H).astype(jnp.int32)
    feature_width = fact_rows.shape[1]
    portions = fact_rows.shape[0] // ROWS_DEV
    stacked = (fact_rows.reshape(portions, ROWS_DEV, feature_width),
               light_key.reshape(portions, ROWS_DEV),
               heavy_index.reshape(portions, ROWS_DEV))

    def advance(accums, portion):
        values, light_part, heavy_part = portion
        widened = values.astype(jnp.float32)
        light_acc = accums[0].at[light_part].add(widened, mode="drop")
        heavy_acc = accums[1].at[heavy_part].add(widened, mode="drop")
        return (light_acc, heavy_acc), None

    start_state = (jnp.zeros((light_count, feature_width), jnp.float32),
                   jnp.zeros((H, feature_width), jnp.float32))
    (light_sums, heavy_sums), _ = lax.scan(advance, start_state, stacked)
    light_joined = (light_sums * light_dims.astype(jnp.float32)).astype(jnp.bfloat16)
    heavy_joined = (heavy_sums * heavy_dims.astype(jnp.float32)).astype(jnp.bfloat16)
    return light_joined, heavy_joined
```

```python
import functools

import jax
import jax.numpy as jnp
from jax import lax
from jax.experimental import pallas as pl
from jax.experimental.pallas import tpu as pltpu
from jax.sharding import Mesh
from jax.sharding import PartitionSpec as P

ROWS = 4096
F = 512
H = 1024
SLOTS = 1024
CAP = 96
NY, NZ, NC, NX = 4, 8, 2, 4
OWNERS = NY * NZ * NC
SHUFFLE = ("y", "z", "c")
ALL = ("y", "z", "c", "x")
LANES = 128
BLOCKS = ROWS // LANES


def table_kernel(owner_ref, slot_ref, flag_ref, source_ref, key_ref):
    row = lax.broadcasted_iota(jnp.int32, (LANES, 2 * LANES), 0)
    col = lax.broadcasted_iota(jnp.int32, (LANES, 2 * LANES), 1)
    before = jnp.where((row < col) | (col >= LANES), 1.0, 0.0).astype(jnp.bfloat16)
    owner_of = lax.broadcasted_iota(jnp.int32, (OWNERS, LANES), 0)
    rank_of = lax.broadcasted_iota(jnp.int32, (LANES, LANES), 0).astype(jnp.float32)
    lane = lax.broadcasted_iota(jnp.int32, (1, LANES), 1)

    def step(b, carried):
        seen, table = carried
        here = pl.ds(b, 1)
        owner = jnp.where(flag_ref[here, :] == 0, owner_ref[here, :], -1)
        slot = slot_ref[here, :]
        hot = jnp.where(owner_of == owner, 1.0, 0.0)
        hot16 = hot.astype(jnp.bfloat16)
        counts = jnp.dot(hot16, before, preferred_element_type=jnp.float32)
        rank = jnp.sum(hot * (counts[:, :LANES] + seen), axis=0, keepdims=True)
        at_rank = rank_of == rank
        high = lax.shift_right_logical(slot, 8)
        values = (lane + 1, jnp.full((1, LANES), b, jnp.int32), slot - high * 256, high)
        placed = jnp.concatenate(
            [jnp.where(at_rank, value.astype(jnp.float32), 0.0) for value in values], axis=0
        ).astype(jnp.bfloat16)
        found = lax.dot_general(
            hot16, placed, (((1,), (1,)), ((), ())), preferred_element_type=jnp.float32
        )
        return seen + counts[:, LANES:], table + found

    start = (jnp.zeros((OWNERS, LANES), jnp.float32), jnp.zeros((OWNERS, 4 * LANES), jnp.float32))
    _, table = lax.fori_loop(0, BLOCKS, step, start)
    first, block, low, high = (
        table[:, i * LANES : (i + 1) * LANES].astype(jnp.int32) for i in range(4)
    )
    filled = first > 0
    source_ref[...] = jnp.where(filled, (block * LANES + first - 1) * 4, 0)
    key_ref[...] = jnp.where(filled, high * 256 + low, -1)


def tables(owner, slot, flag):
    shape = jax.ShapeDtypeStruct((OWNERS, LANES), jnp.int32)
    return pl.pallas_call(table_kernel, out_shape=(shape, shape), name="tables")(owner, slot, flag)


def heavy_kernel(key_ref, flag_ref, x_ref, out_ref):
    step = pl.program_id(0)
    keys = lax.broadcasted_iota(jnp.int32, (H, LANES), 0)
    total = None
    for b in range(4):
        here = pl.ds(b, 1)
        key = jnp.where(flag_ref[here, :] == 1, key_ref[here, :], -1)
        hot = jnp.where(keys == key, 1.0, 0.0).astype(jnp.bfloat16)
        part = jnp.dot(
            hot, x_ref[b * LANES : (b + 1) * LANES, :], preferred_element_type=jnp.float32
        )
        total = part if total is None else total + part

    @pl.when(step == 0)
    def _():
        out_ref[...] = total

    @pl.when(step > 0)
    def _():
        out_ref[...] += total


def heavy_partial(key, flag, rows):
    steps = BLOCKS // 4
    return pl.pallas_call(
        heavy_kernel,
        grid=(steps,),
        in_specs=[
            pl.BlockSpec((None, 4, LANES), lambda i: (i, 0, 0)),
            pl.BlockSpec((None, 4, LANES), lambda i: (i, 0, 0)),
            pl.BlockSpec((4 * LANES, F), lambda i: (i, 0)),
        ],
        out_specs=pl.BlockSpec((H, F), lambda i: (0, 0)),
        out_shape=jax.ShapeDtypeStruct((H, F), jnp.float32),
        name="heavy_partial",
        cost_estimate=pl.CostEstimate(flops=2 * H * ROWS * F, bytes_accessed=6 << 20, transcendentals=0),
    )(key.reshape(steps, 4, LANES), flag.reshape(steps, 4, LANES), rows)


def gather_kernel(source_ref, x_ref, out_ref, wide, picked):
    z = pl.program_id(0)

    @pl.when(z == 0)
    def _():
        def widen(i, _):
            part = x_ref[pl.ds(pl.multiple_of(i * 64, 64), 64), :]
            for f in range(4):
                wide[pl.ds(i * 256 + f, 64, stride=4), :] = part[
                    :, f * LANES : (f + 1) * LANES
                ].astype(jnp.float32)
            return 0

        lax.fori_loop(0, ROWS // 64, widen, 0)

    for yc in range(8):
        owner = (yc // 2 * NZ + z) * 2 + yc % 2

        def pick(i, _):
            for k in range(16):
                r = i * 16 + k
                start = pl.multiple_of(source_ref[owner, r], 4)
                picked[pl.ds(pl.multiple_of((yc * CAP + r) * 4, 4), 4), :] = wide[pl.ds(start, 4), :]
            return 0

        lax.fori_loop(0, CAP // 16, pick, 0)
    for yc in range(8):
        for f in range(4):
            out_ref[f, yc, 0] = picked[pl.ds(yc * CAP * 4 + f, CAP, stride=4), :].astype(jnp.bfloat16)


def gather(source, rows):
    return pl.pallas_call(
        gather_kernel,
        grid_spec=pltpu.PrefetchScalarGridSpec(
            num_scalar_prefetch=1,
            grid=(NZ,),
            in_specs=[pl.BlockSpec((ROWS, F), lambda z, s: (0, 0))],
            out_specs=pl.BlockSpec((4, 8, 1, CAP, LANES), lambda z, s: (0, 0, z, 0, 0)),
            scratch_shapes=[
                pltpu.VMEM((ROWS * 4, LANES), jnp.float32),
                pltpu.VMEM((8 * CAP * 4, LANES), jnp.float32),
            ],
        ),
        out_shape=jax.ShapeDtypeStruct((4, 8, NZ, CAP, LANES), jnp.bfloat16),
        compiler_params=pltpu.CompilerParams(vmem_limit_bytes=60 << 20),
        name="gather_rows",
    )(source, rows)


def light_kernel(key_ref, rows_ref, out_ref):
    keys = lax.broadcasted_iota(jnp.int32, (SLOTS, LANES), 0)
    out_ref[...] = jnp.zeros_like(out_ref)

    def step(k, _):
        lanes = key_ref[0, pl.ds(k, 1), :]
        hot = jnp.where(keys == lanes, 1.0, 0.0).astype(jnp.bfloat16)
        part = rows_ref[0, pl.ds(pl.multiple_of(k * LANES, LANES), LANES), :]
        out_ref[0] += jnp.dot(hot, part, preferred_element_type=jnp.float32)
        return 0

    lax.fori_loop(0, 24, step, 0)


def light_partial(keys, rows):
    return pl.pallas_call(
        light_kernel,
        grid=(NZ,),
        in_specs=[
            pl.BlockSpec((1, 24, LANES), lambda z: (z, 0, 0)),
            pl.BlockSpec((1, 3072, LANES), lambda z: (z, 0, 0)),
        ],
        out_specs=pl.BlockSpec((1, SLOTS, LANES), lambda z: (z, 0, 0)),
        out_shape=jax.ShapeDtypeStruct((NZ, SLOTS, LANES), jnp.float32),
        name="light_partial",
    )(keys, rows)


def shards(rows, owner, slot, flag, heavy_key, light_dims, heavy_dims):
    lane_major = (BLOCKS, LANES)
    owner, slot, flag, heavy_key = (
        value.reshape(lane_major) for value in (owner, slot, flag, heavy_key)
    )
    source, key = tables(owner, slot, flag)
    heavy = heavy_partial(heavy_key, flag, rows)
    buckets = gather(source, rows)
    plane = ("x", "y", "c")
    sent = buckets.reshape(32, NZ * CAP, LANES)
    by_owner = key[:, :CAP].reshape(NY, NZ, NC, CAP).transpose(0, 2, 1, 3).reshape(8, NZ * CAP)
    sent_keys = jnp.broadcast_to(by_owner[None], (4, 8, NZ * CAP)).reshape(32, NZ * CAP)
    came_keys = lax.all_to_all(sent_keys, plane, 0, 0, tiled=True)
    came = lax.all_to_all(sent, plane, 0, 0, tiled=True)
    came = came.reshape(32, NZ, CAP, LANES).transpose(1, 0, 2, 3).reshape(NZ, 32 * CAP, LANES)
    came_keys = came_keys.reshape(32, NZ, CAP).transpose(1, 0, 2).reshape(NZ, 24, LANES)
    partial = light_partial(came_keys, came)
    totals = lax.psum_scatter(partial, "z", scatter_dimension=0, tiled=True)[0]
    light_joined = (totals * light_dims.astype(jnp.float32)).astype(jnp.bfloat16)
    every_dims = lax.all_gather(heavy_dims, ALL, axis=0, tiled=True)
    heavy_sums = lax.psum(heavy, ALL)
    heavy_joined = (heavy_sums * every_dims.astype(jnp.float32)).astype(jnp.bfloat16)
    return light_joined, heavy_joined


def solution(mesh):
    torus = Mesh(mesh.devices.reshape(NY, NZ, NC, NX), ALL)
    rows = P(ALL, None)
    return jax.shard_map(
        shards,
        mesh=torus,
        in_specs=(rows, rows, rows, rows, rows, P(SHUFFLE, "x"), rows),
        out_specs=(P(SHUFFLE, "x"), P()),
        check_vma=False,
    )
```

```python
import functools

import jax
import jax.numpy as jnp
from jax import lax
from jax.experimental import pallas as pl
from jax.experimental.pallas import tpu as pltpu
from jax.sharding import Mesh
from jax.sharding import PartitionSpec as P

ROWS = 4096
F = 512
H = 1024
SLOTS = 1024
CAP = 96
NY, NZ, NC, NX = 4, 8, 2, 4
OWNERS = NY * NZ * NC
SHUFFLE = ("y", "z", "c")
ALL = ("y", "z", "c", "x")
LANES = 128
PLANE = NX * NY * NC
MESH = pl.DeviceIdType.MESH
FAR_FIRST = (4, 3, -3, 2, -2, 1, -1, 0)
HALF = SLOTS // 2


def table_kernel(owner_ref, slot_ref, flag_ref, source_ref, key_ref):
    K = 2 * LANES
    row = lax.broadcasted_iota(jnp.int32, (K, K), 0)
    col = lax.broadcasted_iota(jnp.int32, (K, K), 1)
    before = jnp.where(row < col, 1.0, 0.0).astype(jnp.bfloat16)
    owner_of = lax.broadcasted_iota(jnp.int32, (OWNERS, K), 0)
    rank_of = lax.broadcasted_iota(jnp.int32, (CAP, K), 0).astype(jnp.float32)
    lane = lax.broadcasted_iota(jnp.int32, (1, K), 1)
    ones = jnp.ones((K, LANES), jnp.bfloat16)
    seen = jnp.zeros((OWNERS, 1), jnp.float32)
    table = jnp.zeros((4 * CAP, OWNERS), jnp.float32)
    for b in range(ROWS // K):
        owner = owner_ref[b : b + 1, :]
        owner = (owner >> 4) * 16 + (owner & 1) * 8 + ((owner >> 1) & 7)
        owner = jnp.where(flag_ref[b : b + 1, :] == 0, owner, -1)
        slot = slot_ref[b : b + 1, :]
        hot = jnp.where(owner_of == owner, 1.0, 0.0)
        hot16 = hot.astype(jnp.bfloat16)
        counts = jnp.dot(hot16, before, preferred_element_type=jnp.float32)
        rank = jnp.sum(hot * (counts + seen), axis=0, keepdims=True)
        seen = seen + jnp.sum(hot, axis=1, keepdims=True)
        at_rank = rank_of == rank
        high = lax.shift_right_logical(slot, 8)
        values = ((lane & 127) + 1, 2 * b + (lane >> 7), slot - high * 256, high)
        placed = jnp.concatenate(
            [jnp.where(at_rank, value.astype(jnp.float32), 0.0).astype(jnp.bfloat16) for value in values], axis=0)
        table = table + lax.dot_general(placed, hot16, (((1,), (1,)), ((), ())), preferred_element_type=jnp.float32)
    first, block, low, high = (
        jnp.concatenate([table[i * CAP : (i + 1) * CAP], jnp.zeros((LANES - CAP, OWNERS), jnp.float32)], axis=0).T.astype(jnp.int32) for i in range(4))
    filled = first > 0
    source_ref[...] = jnp.where(filled, block * LANES + first - 1, 0)
    key_ref[...] = jnp.where(filled, high * 256 + low, -1)

def tables(owner, slot, flag):
    shape = jax.ShapeDtypeStruct((OWNERS, LANES), jnp.int32)
    r = lambda v: v.reshape(16, 256)
    return pl.pallas_call(table_kernel, out_shape=(shape, shape), name="tables")(r(owner), r(slot), r(flag))


def fused_kernel(
    source_ref, key_ref, x_ref, out_ref,
    wide, picked, send, recv, keys_in, packed, up_in, down_in, acc,
    key_send, key_recv, row_send, row_recv, up_send, up_recv, down_send, down_recv,
):
    y, z, c, x = (lax.axis_index(name) for name in ALL)
    mine = y * 2 + c

    def peer(d):
        return ((y + d // 2 % 4) % 4, z, (c + d % 2) % 2, (x + d // 8) % 4)

    up, down = (y, (z + 1) % NZ, c, x), (y, (z + NZ - 1) % NZ, c, x)

    def copy_to(target, src, dst, send_sem, recv_sem):
        return pltpu.make_async_remote_copy(
            src_ref=src, dst_ref=dst, send_sem=send_sem, recv_sem=recv_sem,
            device_id=target, device_id_type=MESH,
        )

    barrier = pltpu.get_barrier_semaphore()

    def greet(d, _):
        pl.semaphore_signal(barrier, inc=1, device_id=peer(d), device_id_type=MESH)
        return 0

    lax.fori_loop(1, PLANE, greet, 0)
    for target in (up, down):
        pl.semaphore_signal(barrier, inc=1, device_id=target, device_id_type=MESH)

    def widen(i, _):
        part = x_ref[pl.ds(pl.multiple_of(i * 64, 64), 64), :]
        for f in range(4):
            wide[pl.ds(pl.multiple_of(i * 64, 64), 64), f, :] = part[:, f * LANES : (f + 1) * LANES].astype(
                jnp.float32
            )
        return 0

    lax.fori_loop(0, ROWS // 64, widen, 0)

    def gather(q):
        plane = (z + FAR_FIRST[q] + NZ) % NZ

        def pick(yc, _):
            base = pl.multiple_of(yc * CAP * 4, 4)
            for first in range(0, CAP, 16):
                got = [
                    wide[source_ref[yc * NZ + plane, first + k]]
                    for k in range(16)
                ]
                for k in range(16):
                    picked[pl.ds(base + (first + k) * 4, 4), :] = got[k]
            return 0

        lax.fori_loop(0, 8, pick, 0)

        def narrow(yc, _):
            for f in range(4):
                send[q, f, yc] = picked[pl.ds(yc * CAP * 4 + f, CAP, stride=4), :].astype(jnp.bfloat16)
            return 0

        lax.fori_loop(0, 8, narrow, 0)
        recv[q, 0:CAP, :] = send[q, x, mine]

    def start_rows(q):
        def go(d, _):
            target = peer(d)
            copy_to(
                target,
                send.at[q, target[3], target[0] * 2 + target[2]],
                recv.at[q, pl.ds(pl.multiple_of(d * CAP, CAP), CAP)],
                row_send.at[q], row_recv.at[q],
            ).start()
            return 0

        lax.fori_loop(1, PLANE, go, 0)

    def rows_of(q):
        rest = recv.at[q, pl.ds(CAP, (PLANE - 1) * CAP)]
        return copy_to(peer(1), rest, rest, row_send.at[q], row_recv.at[q])

    gather(0)
    pl.semaphore_wait(barrier, PLANE + 1)

    def send_keys(d, _):
        target = peer(d)
        copy_to(target, key_ref.at[target[0] * 2 + target[2]], keys_in.at[d], key_send, key_recv).start()
        return 0

    lax.fori_loop(1, PLANE, send_keys, 0)
    start_rows(0)
    keys_in[0] = key_ref[mine]
    gather(1)
    start_rows(1)
    gather(2)
    start_rows(2)

    all_keys = copy_to(peer(1), keys_in.at[pl.ds(1, PLANE - 1)], keys_in.at[pl.ds(1, PLANE - 1)], key_send, key_recv)
    all_keys.wait_recv()
    lane = lax.broadcasted_iota(jnp.int32, (NZ, LANES), 1)
    for m in range(PLANE // 4):
        k0, k1, k2, k3 = (keys_in[4 * m + i] for i in range(4))
        k1, k2, k3 = pltpu.roll(k1, 96, 1), pltpu.roll(k2, 64, 1), pltpu.roll(k3, 32, 1)
        packed[3 * m] = jnp.where(lane < 96, k0, k1)
        packed[3 * m + 1] = jnp.where(lane < 64, k1, k2)
        packed[3 * m + 2] = jnp.where(lane < 32, k2, k3)

    block = 768
    tiles = block // LANES
    slot_of = lax.broadcasted_iota(jnp.int32, (SLOTS, block), 0)

    def add_up(q):
        plane = (z + FAR_FIRST[q] + NZ) % NZ
        rows_of(q).wait_recv()

        def part(k):
            lanes = jnp.concatenate(
                [packed[k * tiles + i, pl.ds(plane, 1), :] for i in range(tiles)], axis=1
            )
            hot = jnp.where(slot_of == lanes, 1.0, 0.0).astype(jnp.bfloat16)
            rows = recv[q, pl.ds(pl.multiple_of(k * block, block), block), :]
            return jnp.dot(hot, rows, preferred_element_type=jnp.float32)

        acc[q] = part(0)

        def step(k, _):
            acc[q] += part(k)
            return 0

        lax.fori_loop(1, PLANE * CAP // block, step, 0)

    low, high, whole = pl.ds(0, HALF), pl.ds(HALF, HALF), pl.ds(0, SLOTS)

    def up_copy(q, r, part):
        return copy_to(up, acc.at[q, part], up_in.at[r - 1, part], up_send.at[r - 1], up_recv.at[r - 1])

    def down_copy(q, r, part):
        return copy_to(down, acc.at[q, part], down_in.at[r - 1, part], down_send.at[r - 1], down_recv.at[r - 1])

    for q, r in enumerate(FAR_FIRST):
        if q + 3 < len(FAR_FIRST):
            gather(q + 3)
            start_rows(q + 3)
        add_up(q)
        if r == 4:
            up_copy(q, 4, low).start()
            down_copy(q, 4, high).start()
        elif r > 0:
            part = low if r == 3 else whole
            up_copy(0, r + 1, part).wait_recv()
            acc[q, part, :] += up_in[r, part, :]
            up_copy(q, r, whole).start()
        elif r < 0:
            part = high if r == -3 else whole
            down_copy(0, 1 - r, part).wait_recv()
            acc[q, part, :] += down_in[-r, part, :]
            down_copy(q, -r, whole).start()
        else:
            up_copy(0, 1, whole).wait_recv()
            down_copy(0, 1, whole).wait_recv()
            out_ref[...] = acc[q] + up_in[0] + down_in[0]

    all_keys.wait_send()
    for q in range(len(FAR_FIRST)):
        rows_of(q).wait_send()
    for r in range(1, 5):
        up_copy(0, r, low if r == 4 else whole).wait_send()
        down_copy(0, r, high if r == 4 else whole).wait_send()


def light_totals(source, key, rows):
    vmem = pl.BlockSpec(memory_space=pltpu.VMEM)
    dma = pltpu.SemaphoreType.DMA
    return pl.pallas_call(
        fused_kernel,
        in_specs=[pl.BlockSpec(memory_space=pltpu.SMEM), vmem, vmem],
        out_specs=vmem,
        out_shape=jax.ShapeDtypeStruct((SLOTS, LANES), jnp.float32),
        scratch_shapes=[
            pltpu.VMEM((ROWS, 4, LANES), jnp.float32),
            pltpu.VMEM((8 * CAP * 4, LANES), jnp.float32),
            pltpu.VMEM((NZ, NX, 8, CAP, LANES), jnp.bfloat16),
            pltpu.VMEM((NZ, PLANE * CAP, LANES), jnp.bfloat16),
            pltpu.VMEM((PLANE, NZ, LANES), jnp.int32),
            pltpu.VMEM((PLANE * CAP // LANES, NZ, LANES), jnp.int32),
            pltpu.VMEM((4, SLOTS, LANES), jnp.float32),
            pltpu.VMEM((4, SLOTS, LANES), jnp.float32),
            pltpu.VMEM((NZ, SLOTS, LANES), jnp.float32),
            dma, dma, dma((NZ,)), dma((NZ,)), dma((4,)), dma((4,)), dma((4,)), dma((4,)),
        ],
        compiler_params=pltpu.CompilerParams(
            collective_id=0, has_side_effects=True, vmem_limit_bytes=62 << 20
        ),
        name="light_totals",
    )(source, key.reshape(8, NZ, LANES), rows)


def split_up(value, dim, count):
    dims = value.shape
    pieces = value.reshape(*dims[:dim], count, dims[dim] // count, *dims[dim + 1 :])
    return jnp.moveaxis(pieces, dim, 0)


def sum_at_owner(value, axis, dim):
    count = lax.axis_size(axis)
    pieces = lax.all_to_all(split_up(value, dim, count), axis, 0, 0, tiled=True)
    return jnp.sum(pieces, axis=0)


def summed_rows(value, axes, dim):
    far, near = axes
    pieces = split_up(value, dim, lax.axis_size(far))
    nearer = sum_at_owner(pieces, near, dim + 1)
    arrived = lax.all_to_all(nearer, far, split_axis=0, concat_axis=0, tiled=True)
    return arrived.sum(axis=0)


def heavy_kernel(key_ref, x_ref, out_ref):
    slot_of = lax.broadcasted_iota(jnp.int32, (H, 512), 0)
    lanes = jnp.concatenate([key_ref[0, i : i + 1, :] for i in range(4)], axis=1)
    hot = jnp.where(slot_of == lanes, 1.0, 0.0).astype(jnp.bfloat16)
    part = jnp.dot(hot, x_ref[...], preferred_element_type=jnp.float32)

    @pl.when(pl.program_id(0) == 0)
    def _():
        out_ref[...] = part

    @pl.when(pl.program_id(0) > 0)
    def _():
        out_ref[...] += part


def heavy_partial(key, rows):
    return pl.pallas_call(
        heavy_kernel,
        grid=(8,),
        in_specs=[
            pl.BlockSpec((1, 4, LANES), lambda i: (i, 0, 0)),
            pl.BlockSpec((512, F), lambda i: (i, 0)),
        ],
        out_specs=pl.BlockSpec((H, F), lambda i: (0, 0)),
        out_shape=jax.ShapeDtypeStruct((H, F), jnp.float32),
        name="heavy_partial",
    )(key.reshape(8, 4, LANES), rows)


def shards(rows, owner, slot, flag, heavy_key, light_dims, heavy_dims):
    owner, slot, flag, heavy_key = (v.reshape(ROWS) for v in (owner, slot, flag, heavy_key))
    source, key = tables(owner, slot, flag)
    totals = light_totals(source, key, rows)
    light_joined = (totals * light_dims.astype(jnp.float32)).astype(jnp.bfloat16)
    heavy = heavy_partial(jnp.where(flag == 1, heavy_key, -1), rows)
    shares = summed_rows(heavy, (("y", "z"), ("c", "x")), 0)
    joined_here = (shares * heavy_dims.astype(jnp.float32)).astype(jnp.bfloat16)
    heavy_joined = lax.all_gather(joined_here, ALL, axis=0, tiled=True)
    return light_joined, heavy_joined


def solution(mesh):
    torus = Mesh(mesh.devices.reshape(NY, NZ, NC, NX), ALL)
    rows = P(ALL, None)
    return jax.shard_map(
        shards,
        mesh=torus,
        in_specs=(rows, rows, rows, rows, rows, P(SHUFFLE, "x"), rows),
        out_specs=(P(SHUFFLE, "x"), P()),
        check_vma=False,
    )
```

```python
import functools

import jax
import jax.numpy as jnp
from jax import lax
from jax.experimental import pallas as pl
from jax.experimental.pallas import tpu as pltpu
from jax.sharding import Mesh
from jax.sharding import PartitionSpec as P

ROWS = 4096
F = 512
H = 1024
SLOTS = 1024
CAP = 96
NY, NZ, NC, NX = 4, 8, 2, 4
OWNERS = NY * NZ * NC
SHUFFLE = ("y", "z", "c")
ALL = ("y", "z", "c", "x")
LANES = 128
PLANE = NX * NY * NC
MESH = pl.DeviceIdType.MESH
FAR_FIRST = (4, 3, -3, 2, -2, 1, -1, 0)
HALF = SLOTS // 2


def table_kernel(owner_ref, slot_ref, flag_ref, source_ref, key_ref):
    K = 2 * LANES
    row = lax.broadcasted_iota(jnp.int32, (K, K), 0)
    col = lax.broadcasted_iota(jnp.int32, (K, K), 1)
    before = jnp.where(row < col, 1.0, 0.0).astype(jnp.bfloat16)
    owner_of = lax.broadcasted_iota(jnp.int32, (OWNERS, K), 0)
    rank_of = lax.broadcasted_iota(jnp.int32, (CAP, K), 0).astype(jnp.float32)
    lane = lax.broadcasted_iota(jnp.int32, (1, K), 1)
    ones = jnp.ones((K, LANES), jnp.bfloat16)
    seen = jnp.zeros((OWNERS, 1), jnp.float32)
    table = jnp.zeros((4 * CAP, OWNERS), jnp.float32)
    for b in range(ROWS // K):
        owner, slot, flag = (
            jnp.concatenate([ref[2 * b : 2 * b + 1, :], ref[2 * b + 1 : 2 * b + 2, :]], axis=1)
            for ref in (owner_ref, slot_ref, flag_ref)
        )
        owner = (owner >> 4) * 16 + (owner & 1) * 8 + ((owner >> 1) & 7)
        owner = jnp.where(flag == 0, owner, -1)
        hot = jnp.where(owner_of == owner, 1.0, 0.0)
        hot16 = hot.astype(jnp.bfloat16)
        counts = jnp.dot(hot16, before, preferred_element_type=jnp.float32)
        rank = jnp.sum(hot * (counts + seen), axis=0, keepdims=True)
        seen = seen + jnp.sum(hot, axis=1, keepdims=True)
        at_rank = rank_of == rank
        high = lax.shift_right_logical(slot, 8)
        values = ((lane & 127) + 1, 2 * b + (lane >> 7), slot - high * 256, high)
        placed = jnp.concatenate(
            [jnp.where(at_rank, value.astype(jnp.float32), 0.0).astype(jnp.bfloat16) for value in values], axis=0)
        table = table + lax.dot_general(placed, hot16, (((1,), (1,)), ((), ())), preferred_element_type=jnp.float32)
    first, block, low, high = (
        jnp.concatenate([table[i * CAP : (i + 1) * CAP], jnp.zeros((LANES - CAP, OWNERS), jnp.float32)], axis=0).T.astype(jnp.int32) for i in range(4))
    filled = first > 0
    source_ref[...] = jnp.where(filled, block * LANES + first - 1, 0)
    key_ref[...] = jnp.where(filled, high * 256 + low, -1)

def tables(owner, slot, flag):
    shape = jax.ShapeDtypeStruct((OWNERS, LANES), jnp.int32)
    return pl.pallas_call(table_kernel, out_shape=(shape, shape), name="tables")(owner, slot, flag)


def fused_kernel(
    source_ref, key_ref, hkey_ref, flag_ref, x_ref, dims_ref, hdims_ref, out_ref, hout,
    wide, picked, send, recv, keys_in, packed, up_in, down_in, acc,
    hacc, half_in, hrun, hup_in, hdown_in, hpart, plane_in,
    key_send, key_recv, row_send, row_recv, up_send, up_recv, down_send, down_recv,
    half_send, half_recv, hup_send, hup_recv, hdown_send, hdown_recv, part_send, part_recv,
    line_send, line_recv, sheet_send, sheet_recv, twin_send, twin_recv,
):
    y, z, c, x = (lax.axis_index(name) for name in ALL)
    mine = y * 2 + c

    def peer(d):
        return ((y + d // 2 % 4) % 4, z, (c + d % 2) % 2, (x + d // 8) % 4)

    up, down = (y, (z + 1) % NZ, c, x), (y, (z + NZ - 1) % NZ, c, x)

    def copy_to(target, src, dst, send_sem, recv_sem):
        return pltpu.make_async_remote_copy(
            src_ref=src, dst_ref=dst, send_sem=send_sem, recv_sem=recv_sem,
            device_id=target, device_id_type=MESH,
        )

    barrier = pltpu.get_barrier_semaphore()

    def greet(d, _):
        pl.semaphore_signal(barrier, inc=1, device_id=peer(d), device_id_type=MESH)
        return 0

    lax.fori_loop(1, PLANE, greet, 0)

    def along(d):
        return (y, (z + d) % NZ, c, x)

    def across(d):
        return ((y + d % 4) % 4, z, c, (x + d // 4) % 4)

    twin = (y, z, 1 - c, x)

    def greet_line(d, _):
        pl.semaphore_signal(barrier, inc=1, device_id=along(d), device_id_type=MESH)
        return 0

    lax.fori_loop(1, NZ, greet_line, 0)

    def widen(i, _):
        part = x_ref[pl.ds(pl.multiple_of(i * 64, 64), 64), :]
        for f in range(4):
            wide[pl.ds(pl.multiple_of(i * 64, 64), 64), f, :] = part[:, f * LANES : (f + 1) * LANES].astype(
                jnp.float32
            )
        return 0

    lax.fori_loop(0, ROWS // 64, widen, 0)

    def gather(q):
        plane = (z + FAR_FIRST[q] + NZ) % NZ

        def pick(yc, _):
            base = pl.multiple_of(yc * CAP * 4, 4)
            for first in range(0, CAP, 16):
                got = [
                    wide[source_ref[yc * NZ + plane, first + k]]
                    for k in range(16)
                ]
                for k in range(16):
                    picked[pl.ds(base + (first + k) * 4, 4), :] = got[k]
            return 0

        lax.fori_loop(0, 8, pick, 0)

        def narrow(yc, _):
            for f in range(4):
                send[q, f, yc] = picked[pl.ds(yc * CAP * 4 + f, CAP, stride=4), :].astype(jnp.bfloat16)
            return 0

        lax.fori_loop(0, 8, narrow, 0)
        recv[q, 0:CAP, :] = send[q, x, mine]

    def start_rows(q):
        def go(d, _):
            target = peer(d)
            copy_to(
                target,
                send.at[q, target[3], target[0] * 2 + target[2]],
                recv.at[q, pl.ds(pl.multiple_of(d * CAP, CAP), CAP)],
                row_send.at[q], row_recv.at[q],
            ).start()
            return 0

        lax.fori_loop(1, PLANE, go, 0)

    def rows_of(q):
        rest = recv.at[q, pl.ds(CAP, (PLANE - 1) * CAP)]
        return copy_to(peer(1), rest, rest, row_send.at[q], row_recv.at[q])

    gather(0)
    pl.semaphore_wait(barrier, PLANE + NZ - 2)

    def send_keys(d, _):
        target = peer(d)
        copy_to(target, key_ref.at[target[0] * 2 + target[2]], keys_in.at[d], key_send, key_recv).start()
        return 0

    lax.fori_loop(1, PLANE, send_keys, 0)
    start_rows(0)
    keys_in[0] = key_ref[mine]
    gather(1)
    start_rows(1)

    heavy_of = lax.broadcasted_iota(jnp.int32, (H, F), 0)

    def heavy_block(b):
        lanes = []
        for i in range(4):
            k = hkey_ref[pl.ds(b * 4 + i, 1), :]
            k = ((k >> 4) & 1) * 512 + ((k >> 5) & 7) * 64 + (k >> 8) * 16 + (k & 15)
            lanes.append(jnp.where(flag_ref[pl.ds(b * 4 + i, 1), :] == 1, k, -1))
        hot = jnp.where(heavy_of == jnp.concatenate(lanes, axis=1), 1.0, 0.0).astype(jnp.bfloat16)
        rows = x_ref[pl.ds(pl.multiple_of(b * 512, 512), 512), :]
        return jnp.dot(hot, rows, preferred_element_type=jnp.float32)

    hacc[...] = heavy_block(0)

    def heavy_step(b, _):
        hacc[...] += heavy_block(b)
        return 0

    lax.fori_loop(1, ROWS // 512, heavy_step, 0)
    halves = H // 2
    half_copy = copy_to(
        twin, hacc.at[pl.ds(pl.multiple_of((1 - c) * halves, halves), halves)], half_in, half_send, half_recv
    )
    half_copy.start()

    all_keys = copy_to(peer(1), keys_in.at[pl.ds(1, PLANE - 1)], keys_in.at[pl.ds(1, PLANE - 1)], key_send, key_recv)
    all_keys.wait_recv()
    lane = lax.broadcasted_iota(jnp.int32, (NZ, LANES), 1)
    for m in range(PLANE // 4):
        k0, k1, k2, k3 = (keys_in[4 * m + i] for i in range(4))
        k1, k2, k3 = pltpu.roll(k1, 96, 1), pltpu.roll(k2, 64, 1), pltpu.roll(k3, 32, 1)
        packed[3 * m] = jnp.where(lane < 96, k0, k1)
        packed[3 * m + 1] = jnp.where(lane < 64, k1, k2)
        packed[3 * m + 2] = jnp.where(lane < 32, k2, k3)

    block = 768
    tiles = block // LANES
    slot_of = lax.broadcasted_iota(jnp.int32, (SLOTS, block), 0)

    def add_up(q):
        plane = (z + FAR_FIRST[q] + NZ) % NZ
        rows_of(q).wait_recv()

        def part(k):
            lanes = jnp.concatenate(
                [packed[k * tiles + i, pl.ds(plane, 1), :] for i in range(tiles)], axis=1
            )
            hot = jnp.where(slot_of == lanes, 1.0, 0.0).astype(jnp.bfloat16)
            rows = recv[q, pl.ds(pl.multiple_of(k * block, block), block), :]
            return jnp.dot(hot, rows, preferred_element_type=jnp.float32)

        acc[q] = part(0)

        def step(k, _):
            acc[q] += part(k)
            return 0

        lax.fori_loop(1, PLANE * CAP // block, step, 0)

    low, high, whole = pl.ds(0, HALF), pl.ds(HALF, HALF), pl.ds(0, SLOTS)

    def up_copy(q, r, part):
        return copy_to(up, acc.at[q, part], up_in.at[r - 1, part], up_send.at[r - 1], up_recv.at[r - 1])

    def down_copy(q, r, part):
        return copy_to(down, acc.at[q, part], down_in.at[r - 1, part], down_send.at[r - 1], down_recv.at[r - 1])

    hlow, hhigh, hwhole = pl.ds(0, 32), pl.ds(32, 32), pl.ds(0, 64)

    def hup_copy(r, part):
        return copy_to(
            up, hrun.at[(z + r) % NZ, part], hup_in.at[r - 1, part], hup_send.at[r - 1], hup_recv.at[r - 1]
        )

    def hdown_copy(r, part):
        return copy_to(
            down, hrun.at[(z + NZ - r) % NZ, part], hdown_in.at[r - 1, part],
            hdown_send.at[r - 1], hdown_recv.at[r - 1],
        )

    def heavy_far():
        half_copy.wait_recv()

        def own(i, _):
            rows = pl.ds(pl.multiple_of(i * 64, 64), 64)
            hrun[i] = hacc[pl.ds(pl.multiple_of(c * halves + i * 64, 64), 64), :] + half_in[rows, :]
            return 0

        lax.fori_loop(0, NZ, own, 0)
        hup_copy(4, hlow).start()
        hdown_copy(4, hhigh).start()

    def heavy_on(r):
        part = hlow if r == 3 else hwhole
        hup_copy(r + 1, part).wait_recv()
        hrun[(z + r) % NZ, part, :] += hup_in[r, part, :]
        hup_copy(r, hwhole).start()
        part = hhigh if r == 3 else hwhole
        hdown_copy(r + 1, part).wait_recv()
        hrun[(z + NZ - r) % NZ, part, :] += hdown_in[r, part, :]
        hdown_copy(r, hwhole).start()

    def part_copy(d):
        target = across(d)
        return copy_to(
            target, hpart.at[target[0] * 4 + target[3]], plane_in.at[d], part_send.at[d], part_recv.at[d]
        )

    def heavy_plane():
        hup_copy(1, hwhole).wait_recv()
        hdown_copy(1, hwhole).wait_recv()
        hrun[z] += hup_in[0] + hdown_in[0]
        for i in range(16):
            hpart[i] = hrun[z, pl.ds(4 * i, 4), :]
        lax.fori_loop(1, 16, lambda d, _: (part_copy(d).start(), 0)[1], 0)

    def line_copy(d):
        return copy_to(
            along(d), hout.at[y, z, c, x], hout.at[y, z, c, x], line_send.at[d], line_recv.at[d]
        )

    def line_from(d):
        spot = hout.at[y, (z + NZ - d) % NZ, c, x]
        return copy_to(along(d), spot, spot, line_send.at[d], line_recv.at[d])

    def heavy_join():
        lax.fori_loop(1, 16, lambda d, _: (part_copy(d).wait_recv(), 0)[1], 0)
        total = hpart[y * 4 + x]
        for d in range(1, 16):
            total += plane_in[d]
        hout[y, z, c, x] = (total * hdims_ref[...].astype(jnp.float32)).astype(jnp.bfloat16)
        lax.fori_loop(1, NZ, lambda d, _: (line_copy(d).start(), 0)[1], 0)

    def sheet_copy(d):
        spot = hout.at[y, :, c, x]
        return copy_to(across(d), spot, spot, sheet_send.at[d], sheet_recv.at[d])

    def sheet_from(d):
        spot = hout.at[(y + 4 - d % 4) % 4, :, c, (x + 4 - d // 4) % 4]
        return copy_to(across(d), spot, spot, sheet_send.at[d], sheet_recv.at[d])

    def heavy_sheet():
        lax.fori_loop(1, NZ, lambda d, _: (line_from(d).wait_recv(), 0)[1], 0)
        lax.fori_loop(1, 16, lambda d, _: (sheet_copy(d).start(), 0)[1], 0)

    def twin_copy(core):
        spot = hout.at[:, :, core]
        return copy_to(twin, spot, spot, twin_send, twin_recv)

    def heavy_twin():
        lax.fori_loop(1, 16, lambda d, _: (sheet_from(d).wait_recv(), 0)[1], 0)
        twin_copy(c).start()

    ahead = {
        0: heavy_far,
        1: lambda: heavy_on(2),
        2: heavy_plane,
        5: heavy_join,
    }
    behind = {
        0: lambda: heavy_on(3),
        1: lambda: heavy_on(1),
        6: heavy_sheet,
        7: heavy_twin,
    }

    for q, r in enumerate(FAR_FIRST):
        if q in ahead:
            ahead[q]()
        if q + 2 < len(FAR_FIRST):
            gather(q + 2)
            start_rows(q + 2)
        add_up(q)
        if r == 4:
            up_copy(q, 4, low).start()
            down_copy(q, 4, high).start()
        elif r > 0:
            part = low if r == 3 else whole
            up_copy(0, r + 1, part).wait_recv()
            acc[q, part, :] += up_in[r, part, :]
            up_copy(q, r, whole).start()
        elif r < 0:
            part = high if r == -3 else whole
            down_copy(0, 1 - r, part).wait_recv()
            acc[q, part, :] += down_in[-r, part, :]
            down_copy(q, -r, whole).start()
        else:
            up_copy(0, 1, whole).wait_recv()
            down_copy(0, 1, whole).wait_recv()
            total = acc[q] + up_in[0] + down_in[0]
            out_ref[...] = (total * dims_ref[...].astype(jnp.float32)).astype(jnp.bfloat16)
        if q in behind:
            behind[q]()

    twin_copy(1 - c).wait_recv()
    twin_copy(c).wait_send()
    half_copy.wait_send()
    lax.fori_loop(1, 16, lambda d, _: (part_copy(d).wait_send(), 0)[1], 0)
    lax.fori_loop(1, 16, lambda d, _: (sheet_copy(d).wait_send(), 0)[1], 0)
    lax.fori_loop(1, NZ, lambda d, _: (line_copy(d).wait_send(), 0)[1], 0)
    all_keys.wait_send()
    for q in range(len(FAR_FIRST)):
        rows_of(q).wait_send()
    for r in range(1, 5):
        up_copy(0, r, low if r == 4 else whole).wait_send()
        down_copy(0, r, high if r == 4 else whole).wait_send()
        hup_copy(r, hlow if r == 4 else hwhole).wait_send()
        hdown_copy(r, hhigh if r == 4 else hwhole).wait_send()


def join(source, key, heavy_key, flag, rows, light_dims, heavy_dims):
    vmem = pl.BlockSpec(memory_space=pltpu.VMEM)
    dma = pltpu.SemaphoreType.DMA
    f32 = jnp.float32
    return pl.pallas_call(
        fused_kernel,
        in_specs=[pl.BlockSpec(memory_space=pltpu.SMEM)] + [vmem] * 6,
        out_specs=(vmem, vmem),
        out_shape=(
            jax.ShapeDtypeStruct((SLOTS, LANES), jnp.bfloat16),
            jax.ShapeDtypeStruct((NY, NZ, NC, NX, 4, F), jnp.bfloat16),
        ),
        scratch_shapes=[
            pltpu.VMEM((ROWS, 4, LANES), f32),
            pltpu.VMEM((8 * CAP * 4, LANES), f32),
            pltpu.VMEM((NZ, NX, 8, CAP, LANES), jnp.bfloat16),
            pltpu.VMEM((NZ, PLANE * CAP, LANES), jnp.bfloat16),
            pltpu.VMEM((PLANE, NZ, LANES), jnp.int32),
            pltpu.VMEM((PLANE * CAP // LANES, NZ, LANES), jnp.int32),
            pltpu.VMEM((4, SLOTS, LANES), f32),
            pltpu.VMEM((4, SLOTS, LANES), f32),
            pltpu.VMEM((NZ, SLOTS, LANES), f32),
            pltpu.VMEM((H, F), f32),
            pltpu.VMEM((H // 2, F), f32),
            pltpu.VMEM((NZ, 64, F), f32),
            pltpu.VMEM((4, 64, F), f32),
            pltpu.VMEM((4, 64, F), f32),
            pltpu.VMEM((16, 4, F), f32),
            pltpu.VMEM((16, 4, F), f32),
            dma, dma, dma((NZ,)), dma((NZ,)), dma((4,)), dma((4,)), dma((4,)), dma((4,)),
            dma, dma, dma((4,)), dma((4,)), dma((4,)), dma((4,)), dma((16,)), dma((16,)),
            dma((NZ,)), dma((NZ,)), dma((16,)), dma((16,)), dma, dma,
        ],
        compiler_params=pltpu.CompilerParams(
            collective_id=0, has_side_effects=True, vmem_limit_bytes=62 << 20
        ),
        name="join",
    )(source, key.reshape(8, NZ, LANES), heavy_key, flag, rows, light_dims, heavy_dims)


def shards(rows, owner, slot, flag, heavy_key, light_dims, heavy_dims):
    owner, slot, flag, heavy_key = (
        v.reshape(ROWS // LANES, LANES) for v in (owner, slot, flag, heavy_key)
    )
    source, key = tables(owner, slot, flag)
    light_joined, heavy_joined = join(source, key, heavy_key, flag, rows, light_dims, heavy_dims)
    return light_joined, heavy_joined.reshape(H, F)


def solution(mesh):
    torus = Mesh(mesh.devices.reshape(NY, NZ, NC, NX), ALL)
    rows = P(ALL, None)
    return jax.shard_map(
        shards,
        mesh=torus,
        in_specs=(rows, rows, rows, rows, rows, P(SHUFFLE, "x"), rows),
        out_specs=(P(SHUFFLE, "x"), P()),
        check_vma=False,
    )
```

```python
import functools

import jax
import jax.numpy as jnp
from jax import lax
from jax.experimental import pallas as pl
from jax.experimental.pallas import tpu as pltpu
from jax.sharding import Mesh
from jax.sharding import PartitionSpec as P

ROWS = 4096
F = 512
H = 1024
SLOTS = 1024
CAP = 96
NY, NZ, NC, NX = 4, 8, 2, 4
OWNERS = NY * NZ * NC
SHUFFLE = ("y", "z", "c")
ALL = ("y", "z", "c", "x")
LANES = 128
PLANE = NX * NY * NC
MESH = pl.DeviceIdType.MESH
FAR_FIRST = (4, 3, -3, 2, -2, 1, -1, 0)
HALF = SLOTS // 2
X_PART = 256


def table_kernel(owner_ref, slot_ref, flag_ref, source_ref, key_ref):
    K = 2 * LANES
    row = lax.broadcasted_iota(jnp.int32, (K, K), 0)
    col = lax.broadcasted_iota(jnp.int32, (K, K), 1)
    before = jnp.where(row < col, 1.0, 0.0).astype(jnp.bfloat16)
    owner_of = lax.broadcasted_iota(jnp.int32, (OWNERS, K), 0)
    rank_of = lax.broadcasted_iota(jnp.int32, (CAP, K), 0).astype(jnp.float32)
    lane = lax.broadcasted_iota(jnp.int32, (1, K), 1)
    ones = jnp.ones((K, LANES), jnp.bfloat16)
    seen = jnp.zeros((OWNERS, 1), jnp.float32)
    table = jnp.zeros((4 * CAP, OWNERS), jnp.float32)
    for b in range(ROWS // K):
        owner, slot, flag = (
            jnp.concatenate([ref[2 * b : 2 * b + 1, :], ref[2 * b + 1 : 2 * b + 2, :]], axis=1)
            for ref in (owner_ref, slot_ref, flag_ref)
        )
        owner = (owner >> 4) * 16 + (owner & 1) * 8 + ((owner >> 1) & 7)
        owner = jnp.where(flag == 0, owner, -1)
        hot = jnp.where(owner_of == owner, 1.0, 0.0)
        hot16 = hot.astype(jnp.bfloat16)
        counts = jnp.dot(hot16, before, preferred_element_type=jnp.float32)
        rank = jnp.sum(hot * (counts + seen), axis=0, keepdims=True)
        seen = seen + jnp.sum(hot, axis=1, keepdims=True)
        at_rank = rank_of == rank
        high = lax.shift_right_logical(slot, 8)
        values = ((lane & 127) + 1, 2 * b + (lane >> 7), slot - high * 256, high)
        placed = jnp.concatenate(
            [jnp.where(at_rank, value.astype(jnp.float32), 0.0).astype(jnp.bfloat16) for value in values], axis=0)
        table = table + lax.dot_general(placed, hot16, (((1,), (1,)), ((), ())), preferred_element_type=jnp.float32)
    first, block, low, high = (
        jnp.concatenate([table[i * CAP : (i + 1) * CAP], jnp.zeros((LANES - CAP, OWNERS), jnp.float32)], axis=0).T.astype(jnp.int32) for i in range(4))
    filled = first > 0
    source_ref[...] = jnp.where(filled, block * LANES + first - 1, 0)
    key_ref[...] = jnp.where(filled, high * 256 + low, -1)

def tables(owner, slot, flag):
    shape = jax.ShapeDtypeStruct((OWNERS, LANES), jnp.int32)
    return pl.pallas_call(table_kernel, out_shape=(shape, shape), name="tables")(owner, slot, flag)


def fused_kernel(
    source_ref, key_ref, hkey_ref, flag_ref, x_hbm, dims_ref, hdims_ref, out_ref, hout,
    x_ref, x_sem, wide, picked, send, recv, keys_in, packed, up_in, down_in, acc,
    hacc, half_in, hrun, hup_in, hdown_in, hpart, plane_in,
    key_send, key_recv, row_send, row_recv, up_send, up_recv, down_send, down_recv,
    half_send, half_recv, hup_send, hup_recv, hdown_send, hdown_recv, part_send, part_recv,
    line_send, line_recv, sheet_send, sheet_recv, twin_send, twin_recv,
):
    y, z, c, x = (lax.axis_index(name) for name in ALL)
    mine = y * 2 + c

    def peer(d):
        return ((y + d // 2 % 4) % 4, z, (c + d % 2) % 2, (x + d // 8) % 4)

    up, down = (y, (z + 1) % NZ, c, x), (y, (z + NZ - 1) % NZ, c, x)

    def copy_to(target, src, dst, send_sem, recv_sem):
        return pltpu.make_async_remote_copy(
            src_ref=src, dst_ref=dst, send_sem=send_sem, recv_sem=recv_sem,
            device_id=target, device_id_type=MESH,
        )

    def x_part(i):
        rows = pl.ds(pl.multiple_of(i * X_PART, X_PART), X_PART)
        return pltpu.make_async_copy(x_hbm.at[rows], x_ref.at[rows], x_sem.at[i])

    for i in range(ROWS // X_PART):
        x_part(i).start()
    barrier = pltpu.get_barrier_semaphore()

    def greet(d, _):
        pl.semaphore_signal(barrier, inc=1, device_id=peer(d), device_id_type=MESH)
        return 0

    lax.fori_loop(1, PLANE, greet, 0)

    def along(d):
        return (y, (z + d) % NZ, c, x)

    def across(d):
        return ((y + d % 4) % 4, z, c, (x + d // 4) % 4)

    twin = (y, z, 1 - c, x)

    def greet_line(d, _):
        pl.semaphore_signal(barrier, inc=1, device_id=along(d), device_id_type=MESH)
        return 0

    lax.fori_loop(1, NZ, greet_line, 0)

    def widen(i, _):
        x_part(i).wait()
        for j in range(0, X_PART, 64):
            rows = pl.ds(pl.multiple_of(i * X_PART + j, 64), 64)
            for f in range(4):
                wide[f, rows, :] = x_ref[rows, f * LANES : (f + 1) * LANES].astype(jnp.float32)
        return 0

    lax.fori_loop(0, ROWS // X_PART, widen, 0)

    def gather(q):
        plane = (z + FAR_FIRST[q] + NZ) % NZ

        def pick(yc, _):
            base = pl.multiple_of(yc * CAP, 8)
            for first in range(0, CAP, 8):
                rows = [source_ref[yc * NZ + plane, first + k] for k in range(8)]
                got = [[wide[f, row] for f in range(4)] for row in rows]
                for k in range(8):
                    for f in range(4):
                        picked[f, base + first + k] = got[k][f]
            return 0

        lax.fori_loop(0, 8, pick, 0)

        def narrow(yc, _):
            for f in range(4):
                rows = picked[f, pl.ds(pl.multiple_of(yc * CAP, 8), CAP), :]
                send[q, f, yc] = rows.astype(jnp.bfloat16)
            return 0

        lax.fori_loop(0, 8, narrow, 0)
        recv[q, 0:CAP, :] = send[q, x, mine]

    def start_rows(q):
        def go(d, _):
            target = peer(d)
            copy_to(
                target,
                send.at[q, target[3], target[0] * 2 + target[2]],
                recv.at[q, pl.ds(pl.multiple_of(d * CAP, CAP), CAP)],
                row_send.at[q], row_recv.at[q],
            ).start()
            return 0

        lax.fori_loop(1, PLANE, go, 0)

    def rows_of(q):
        rest = recv.at[q, pl.ds(CAP, (PLANE - 1) * CAP)]
        return copy_to(peer(1), rest, rest, row_send.at[q], row_recv.at[q])

    gather(0)
    pl.semaphore_wait(barrier, PLANE + NZ - 2)

    def send_keys(d, _):
        target = peer(d)
        copy_to(target, key_ref.at[target[0] * 2 + target[2]], keys_in.at[d], key_send, key_recv).start()
        return 0

    start_rows(0)
    lax.fori_loop(1, PLANE, send_keys, 0)
    keys_in[0] = key_ref[mine]
    gather(1)
    start_rows(1)

    heavy_of = lax.broadcasted_iota(jnp.int32, (H, F), 0)

    def heavy_block(b):
        lanes = []
        for i in range(4):
            k = hkey_ref[pl.ds(b * 4 + i, 1), :]
            k = ((k >> 4) & 1) * 512 + ((k >> 5) & 7) * 64 + (k >> 8) * 16 + (k & 15)
            lanes.append(jnp.where(flag_ref[pl.ds(b * 4 + i, 1), :] == 1, k, -1))
        hot = jnp.where(heavy_of == jnp.concatenate(lanes, axis=1), 1.0, 0.0).astype(jnp.bfloat16)
        rows = x_ref[pl.ds(pl.multiple_of(b * 512, 512), 512), :]
        return jnp.dot(hot, rows, preferred_element_type=jnp.float32)

    hacc[...] = heavy_block(0)

    def heavy_step(b, _):
        hacc[...] += heavy_block(b)
        return 0

    lax.fori_loop(1, ROWS // 512, heavy_step, 0)
    halves = H // 2
    half_copy = copy_to(
        twin, hacc.at[pl.ds(pl.multiple_of((1 - c) * halves, halves), halves)], half_in, half_send, half_recv
    )
    half_copy.start()

    all_keys = copy_to(peer(1), keys_in.at[pl.ds(1, PLANE - 1)], keys_in.at[pl.ds(1, PLANE - 1)], key_send, key_recv)

    def pack_keys():
        all_keys.wait_recv()
        lane = lax.broadcasted_iota(jnp.int32, (NZ, LANES), 1)
        for m in range(PLANE // 4):
            k0, k1, k2, k3 = (keys_in[4 * m + i] for i in range(4))
            k1, k2, k3 = pltpu.roll(k1, 96, 1), pltpu.roll(k2, 64, 1), pltpu.roll(k3, 32, 1)
            packed[3 * m] = jnp.where(lane < 96, k0, k1)
            packed[3 * m + 1] = jnp.where(lane < 64, k1, k2)
            packed[3 * m + 2] = jnp.where(lane < 32, k2, k3)

    block = 768
    tiles = block // LANES
    slot_of = lax.broadcasted_iota(jnp.int32, (SLOTS, block), 0)

    def add_up(q):
        plane = (z + FAR_FIRST[q] + NZ) % NZ
        rows_of(q).wait_recv()

        def part(k):
            lanes = jnp.concatenate(
                [packed[k * tiles + i, pl.ds(plane, 1), :] for i in range(tiles)], axis=1
            )
            hot = jnp.where(slot_of == lanes, 1.0, 0.0).astype(jnp.bfloat16)
            rows = recv[q, pl.ds(pl.multiple_of(k * block, block), block), :]
            return jnp.dot(hot, rows, preferred_element_type=jnp.float32)

        acc[q] = part(0)

        def step(k, _):
            acc[q] += part(k)
            return 0

        lax.fori_loop(1, PLANE * CAP // block, step, 0)

    low, high, whole = pl.ds(0, HALF), pl.ds(HALF, HALF), pl.ds(0, SLOTS)

    def up_copy(q, r, part):
        return copy_to(up, acc.at[q, part], up_in.at[r - 1, part], up_send.at[r - 1], up_recv.at[r - 1])

    def down_copy(q, r, part):
        return copy_to(down, acc.at[q, part], down_in.at[r - 1, part], down_send.at[r - 1], down_recv.at[r - 1])

    hlow, hhigh, hwhole = pl.ds(0, 32), pl.ds(32, 32), pl.ds(0, 64)

    def hup_copy(r, part):
        return copy_to(
            up, hrun.at[(z + r) % NZ, part], hup_in.at[r - 1, part], hup_send.at[r - 1], hup_recv.at[r - 1]
        )

    def hdown_copy(r, part):
        return copy_to(
            down, hrun.at[(z + NZ - r) % NZ, part], hdown_in.at[r - 1, part],
            hdown_send.at[r - 1], hdown_recv.at[r - 1],
        )

    def heavy_far():
        half_copy.wait_recv()

        def own(i, _):
            rows = pl.ds(pl.multiple_of(i * 64, 64), 64)
            hrun[i] = hacc[pl.ds(pl.multiple_of(c * halves + i * 64, 64), 64), :] + half_in[rows, :]
            return 0

        lax.fori_loop(0, NZ, own, 0)
        hup_copy(4, hlow).start()
        hdown_copy(4, hhigh).start()

    def heavy_on(r):
        part = hlow if r == 3 else hwhole
        hup_copy(r + 1, part).wait_recv()
        hrun[(z + r) % NZ, part, :] += hup_in[r, part, :]
        hup_copy(r, hwhole).start()
        part = hhigh if r == 3 else hwhole
        hdown_copy(r + 1, part).wait_recv()
        hrun[(z + NZ - r) % NZ, part, :] += hdown_in[r, part, :]
        hdown_copy(r, hwhole).start()

    def part_copy(d):
        target = across(d)
        return copy_to(
            target, hpart.at[target[0] * 4 + target[3]], plane_in.at[d], part_send.at[d], part_recv.at[d]
        )

    def heavy_plane():
        hup_copy(1, hwhole).wait_recv()
        hdown_copy(1, hwhole).wait_recv()
        hrun[z] += hup_in[0] + hdown_in[0]
        for i in range(16):
            hpart[i] = hrun[z, pl.ds(4 * i, 4), :]
        lax.fori_loop(1, 16, lambda d, _: (part_copy(d).start(), 0)[1], 0)

    def line_copy(d):
        return copy_to(
            along(d), hout.at[y, z, c, x], hout.at[y, z, c, x], line_send.at[d], line_recv.at[d]
        )

    def line_from(d):
        spot = hout.at[y, (z + NZ - d) % NZ, c, x]
        return copy_to(along(d), spot, spot, line_send.at[d], line_recv.at[d])

    def heavy_join():
        lax.fori_loop(1, 16, lambda d, _: (part_copy(d).wait_recv(), 0)[1], 0)
        total = hpart[y * 4 + x]
        for d in range(1, 16):
            total += plane_in[d]
        hout[y, z, c, x] = (total * hdims_ref[...].astype(jnp.float32)).astype(jnp.bfloat16)
        lax.fori_loop(1, NZ, lambda d, _: (line_copy(d).start(), 0)[1], 0)

    def sheet_copy(d):
        spot = hout.at[y, :, c, x]
        return copy_to(across(d), spot, spot, sheet_send.at[d], sheet_recv.at[d])

    def sheet_from(d):
        spot = hout.at[(y + 4 - d % 4) % 4, :, c, (x + 4 - d // 4) % 4]
        return copy_to(across(d), spot, spot, sheet_send.at[d], sheet_recv.at[d])

    def heavy_sheet():
        lax.fori_loop(1, NZ, lambda d, _: (line_from(d).wait_recv(), 0)[1], 0)
        lax.fori_loop(1, 16, lambda d, _: (sheet_copy(d).start(), 0)[1], 0)

    def twin_copy(core):
        spot = hout.at[:, :, core]
        return copy_to(twin, spot, spot, twin_send, twin_recv)

    def heavy_twin():
        lax.fori_loop(1, 16, lambda d, _: (sheet_from(d).wait_recv(), 0)[1], 0)
        twin_copy(c).start()

    def chain(q):
        r = FAR_FIRST[q]
        if r == 4:
            up_copy(q, 4, low).start()
            down_copy(q, 4, high).start()
        elif r > 0:
            part = low if r == 3 else whole
            up_copy(0, r + 1, part).wait_recv()
            acc[q, part, :] += up_in[r, part, :]
            up_copy(q, r, whole).start()
        elif r < 0:
            part = high if r == -3 else whole
            down_copy(0, 1 - r, part).wait_recv()
            acc[q, part, :] += down_in[-r, part, :]
            down_copy(q, -r, whole).start()
        else:
            up_copy(0, 1, whole).wait_recv()
            down_copy(0, 1, whole).wait_recv()
            total = acc[q] + up_in[0] + down_in[0]
            out_ref[...] = (total * dims_ref[...].astype(jnp.float32)).astype(jnp.bfloat16)

    def issue(q):
        gather(q)
        start_rows(q)

    issue(2)
    heavy_far()
    gather(3)
    heavy_on(3)
    pack_keys()
    add_up(0)
    heavy_on(2)
    start_rows(3)
    add_up(1)
    heavy_on(1)
    chain(0)
    gather(4)
    heavy_plane()
    start_rows(4)
    add_up(2)
    chain(1)
    chain(2)
    gather(5)
    heavy_join()
    start_rows(5)
    add_up(3)
    issue(6)
    add_up(4)
    chain(3)
    chain(4)
    issue(7)
    heavy_sheet()
    add_up(5)
    chain(5)
    add_up(6)
    chain(6)
    add_up(7)
    heavy_twin()
    chain(7)

    twin_copy(1 - c).wait_recv()
    twin_copy(c).wait_send()
    half_copy.wait_send()
    lax.fori_loop(1, 16, lambda d, _: (part_copy(d).wait_send(), 0)[1], 0)
    lax.fori_loop(1, 16, lambda d, _: (sheet_copy(d).wait_send(), 0)[1], 0)
    lax.fori_loop(1, NZ, lambda d, _: (line_copy(d).wait_send(), 0)[1], 0)
    all_keys.wait_send()
    for q in range(len(FAR_FIRST)):
        rows_of(q).wait_send()
    for r in range(1, 5):
        up_copy(0, r, low if r == 4 else whole).wait_send()
        down_copy(0, r, high if r == 4 else whole).wait_send()
        hup_copy(r, hlow if r == 4 else hwhole).wait_send()
        hdown_copy(r, hhigh if r == 4 else hwhole).wait_send()


def join(source, key, heavy_key, flag, rows, light_dims, heavy_dims):
    vmem = pl.BlockSpec(memory_space=pltpu.VMEM)
    dma = pltpu.SemaphoreType.DMA
    f32 = jnp.float32
    return pl.pallas_call(
        fused_kernel,
        in_specs=[pl.BlockSpec(memory_space=pltpu.SMEM)]
        + [vmem] * 3
        + [pl.BlockSpec(memory_space=pl.ANY)]
        + [vmem] * 2,
        out_specs=(vmem, vmem),
        out_shape=(
            jax.ShapeDtypeStruct((SLOTS, LANES), jnp.bfloat16),
            jax.ShapeDtypeStruct((NY, NZ, NC, NX, 4, F), jnp.bfloat16),
        ),
        scratch_shapes=[
            pltpu.VMEM((ROWS, F), jnp.bfloat16),
            dma((ROWS // X_PART,)),
            pltpu.VMEM((4, ROWS, LANES), f32),
            pltpu.VMEM((4, 8 * CAP, LANES), f32),
            pltpu.VMEM((NZ, NX, 8, CAP, LANES), jnp.bfloat16),
            pltpu.VMEM((NZ, PLANE * CAP, LANES), jnp.bfloat16),
            pltpu.VMEM((PLANE, NZ, LANES), jnp.int32),
            pltpu.VMEM((PLANE * CAP // LANES, NZ, LANES), jnp.int32),
            pltpu.VMEM((4, SLOTS, LANES), f32),
            pltpu.VMEM((4, SLOTS, LANES), f32),
            pltpu.VMEM((NZ, SLOTS, LANES), f32),
            pltpu.VMEM((H, F), f32),
            pltpu.VMEM((H // 2, F), f32),
            pltpu.VMEM((NZ, 64, F), f32),
            pltpu.VMEM((4, 64, F), f32),
            pltpu.VMEM((4, 64, F), f32),
            pltpu.VMEM((16, 4, F), f32),
            pltpu.VMEM((16, 4, F), f32),
            dma, dma, dma((NZ,)), dma((NZ,)), dma((4,)), dma((4,)), dma((4,)), dma((4,)),
            dma, dma, dma((4,)), dma((4,)), dma((4,)), dma((4,)), dma((16,)), dma((16,)),
            dma((NZ,)), dma((NZ,)), dma((16,)), dma((16,)), dma, dma,
        ],
        compiler_params=pltpu.CompilerParams(
            collective_id=0, has_side_effects=True, vmem_limit_bytes=62 << 20
        ),
        name="join",
    )(source, key.reshape(8, NZ, LANES), heavy_key, flag, rows, light_dims, heavy_dims)


def shards(rows, owner, slot, flag, heavy_key, light_dims, heavy_dims):
    owner, slot, flag, heavy_key = (
        v.reshape(ROWS // LANES, LANES) for v in (owner, slot, flag, heavy_key)
    )
    source, key = tables(owner, slot, flag)
    light_joined, heavy_joined = join(source, key, heavy_key, flag, rows, light_dims, heavy_dims)
    return light_joined, heavy_joined.reshape(H, F)


def solution(mesh):
    torus = Mesh(mesh.devices.reshape(NY, NZ, NC, NX), ALL)
    rows = P(ALL, None)
    return jax.shard_map(
        shards,
        mesh=torus,
        in_specs=(rows, rows, rows, rows, rows, P(SHUFFLE, "x"), rows),
        out_specs=(P(SHUFFLE, "x"), P()),
        check_vma=False,
    )
```

```python
import functools

import jax
import jax.numpy as jnp
from jax import lax
from jax.experimental import pallas as pl
from jax.experimental.pallas import tpu as pltpu
from jax.sharding import Mesh
from jax.sharding import PartitionSpec as P

ROWS = 4096
F = 512
H = 1024
SLOTS = 1024
CAP = 96
NY, NZ, NC, NX = 4, 8, 2, 4
OWNERS = NY * NZ * NC
SHUFFLE = ("y", "z", "c")
ALL = ("y", "z", "c", "x")
LANES = 128
PLANE = NX * NY * NC
MESH = pl.DeviceIdType.MESH
FAR_FIRST = (4, 3, -3, 2, -2, 1, -1, 0)
HALF = SLOTS // 2
X_PART = 256


def table_kernel(owner_ref, slot_ref, flag_ref, source_ref, key_ref, hots, ranks):
    K = 2 * LANES
    row = lax.broadcasted_iota(jnp.int32, (K, K), 0)
    col = lax.broadcasted_iota(jnp.int32, (K, K), 1)
    before = jnp.where(row < col, 1.0, 0.0).astype(jnp.bfloat16)
    owner_of = lax.broadcasted_iota(jnp.int32, (OWNERS, K), 0)
    rank_of = lax.broadcasted_iota(jnp.int32, (CAP, K), 0).astype(jnp.float32)
    lane = lax.broadcasted_iota(jnp.int32, (1, K), 1)
    seen = jnp.zeros((OWNERS, 1), jnp.float32)
    table = jnp.zeros((4 * CAP, OWNERS), jnp.float32)

    def two(ref, b):
        return jnp.concatenate([ref[2 * b : 2 * b + 1, :], ref[2 * b + 1 : 2 * b + 2, :]], axis=1)

    for b in range(ROWS // K):
        owner = two(owner_ref, b)
        owner = (owner >> 4) * 16 + (owner & 1) * 8 + ((owner >> 1) & 7)
        owner = jnp.where(two(flag_ref, b) == 0, owner, -1)
        hot = jnp.where(owner_of == owner, 1.0, 0.0)
        hots[b] = hot.astype(jnp.bfloat16)
        counts = jnp.dot(hots[b], before, preferred_element_type=jnp.float32)
        ranks[b : b + 1, :] = jnp.sum(hot * (counts + seen), axis=0, keepdims=True)
        seen = seen + jnp.sum(hot, axis=1, keepdims=True)
    for b in range(ROWS // K):
        slot = two(slot_ref, b)
        at_rank = rank_of == ranks[b : b + 1, :]
        high = lax.shift_right_logical(slot, 8)
        values = ((lane & 127) + 1, 2 * b + (lane >> 7), slot - high * 256, high)
        placed = jnp.concatenate(
            [jnp.where(at_rank, value.astype(jnp.float32), 0.0).astype(jnp.bfloat16) for value in values],
            axis=0,
        )
        table = table + lax.dot_general(
            placed, hots[b], (((1,), (1,)), ((), ())), preferred_element_type=jnp.float32
        )
    first, block, low, high = (
        jnp.concatenate([table[i * CAP : (i + 1) * CAP], jnp.zeros((LANES - CAP, OWNERS), jnp.float32)], axis=0).T.astype(jnp.int32) for i in range(4))
    filled = first > 0
    source_ref[...] = jnp.where(filled, block * LANES + first - 1, 0)
    key_ref[...] = jnp.where(filled, high * 256 + low, -1)

def tables(owner, slot, flag):
    shape = jax.ShapeDtypeStruct((OWNERS, LANES), jnp.int32)
    return pl.pallas_call(table_kernel, out_shape=(shape, shape), name="tables",
        scratch_shapes=[
            pltpu.VMEM((ROWS // 256, OWNERS, 256), jnp.bfloat16),
            pltpu.VMEM((ROWS // 256, 256), jnp.float32),
        ])(owner, slot, flag)


def fused_kernel(
    source_ref, key_hbm, hkey_hbm, flag_hbm, x_hbm, dims_hbm, hdims_hbm, out_ref, hfin_ref,
    key_ref, hkey_ref, flag_ref, dims_ref, hdims_ref, in_sem, hout, x_ref, x_sem, wide, picked, send, recv, keys_in, packed, up_in, down_in, acc,
    hacc, half_in, hrun, hup_in, hdown_in, hpart, plane_in,
    key_send, key_recv, row_send, row_recv, up_send, up_recv, down_send, down_recv,
    half_send, half_recv, hup_send, hup_recv, hdown_send, hdown_recv, part_send, part_recv,
    line_send, line_recv, sheet_send, sheet_recv, twin_send, twin_recv,
):
    y, z, c, x = (lax.axis_index(name) for name in ALL)
    mine = y * 2 + c

    def peer(d):
        return (
            lax.rem(y + lax.rem(lax.div(d, 2), 4), 4), z,
            lax.rem(c + lax.rem(d, 2), 2), lax.rem(x + lax.div(d, 8), 4),
        )

    up, down = (y, (z + 1) % NZ, c, x), (y, (z + NZ - 1) % NZ, c, x)

    def copy_to(target, src, dst, send_sem, recv_sem):
        return pltpu.make_async_remote_copy(
            src_ref=src, dst_ref=dst, send_sem=send_sem, recv_sem=recv_sem,
            device_id=target, device_id_type=MESH,
        )

    def x_part(i):
        rows = pl.ds(pl.multiple_of(i * X_PART, X_PART), X_PART)
        return pltpu.make_async_copy(x_hbm.at[rows], x_ref.at[rows], x_sem.at[i])

    for i in range(ROWS // X_PART):
        x_part(i).start()
    barrier = pltpu.get_barrier_semaphore()

    def along(d):
        return (y, (z + d) % NZ, c, x)

    def across(d):
        return ((y + d % 4) % 4, z, c, (x + d // 4) % 4)

    twin = (y, z, 1 - c, x)

    ys, xs, cs = (
        [lax.rem(at + i, count) for i in range(count)] for at, count in ((y, NY), (x, NX), (c, NC))
    )
    for dx in (2, 1, 3, 0):
        for dy in (2, 1, 3, 0):
            for dc in range(NC):
                if dx or dy or dc:
                    pl.semaphore_signal(
                        barrier, inc=1, device_id=(ys[dy], z, cs[dc], xs[dx]), device_id_type=MESH
                    )
    for dz in (4, 3, 5, 2, 6, 1, 7):
        pl.semaphore_signal(barrier, inc=1, device_id=along(dz), device_id_type=MESH)

    small = [
        pltpu.make_async_copy(src, dst, in_sem.at[i])
        for i, (src, dst) in enumerate(
            (
                (key_hbm, key_ref),
                (hkey_hbm, hkey_ref),
                (flag_hbm, flag_ref),
                (dims_hbm, dims_ref),
                (hdims_hbm, hdims_ref),
            )
        )
    ]
    for copy in small:
        copy.start()

    def widen(i, _):
        x_part(i).wait()
        for j in range(0, X_PART, 64):
            rows = pl.ds(pl.multiple_of(i * X_PART + j, 64), 64)
            for f in range(4):
                wide[f, rows, :] = x_ref[rows, f * LANES : (f + 1) * LANES].astype(jnp.float32)
        return 0

    lax.fori_loop(0, ROWS // X_PART, widen, 0)

    def gather(q):
        plane = (z + FAR_FIRST[q] + NZ) % NZ

        def pick(yc, _):
            base = pl.multiple_of(yc * CAP, 8)
            for first in range(0, CAP, 8):
                rows = [source_ref[yc * NZ + plane, first + k] for k in range(8)]
                got = [[wide[f, row] for f in range(4)] for row in rows]
                for k in range(8):
                    for f in range(4):
                        picked[f, base + first + k] = got[k][f]
            return 0

        lax.fori_loop(0, 8, pick, 0)

        def narrow(yc, _):
            for f in range(4):
                rows = picked[f, pl.ds(pl.multiple_of(yc * CAP, 8), CAP), :]
                send[q, f, yc] = rows.astype(jnp.bfloat16)
            return 0

        lax.fori_loop(0, 8, narrow, 0)
        recv[q, 0:CAP, :] = send[q, x, mine]

    def start_rows(q):
        def go(d, _):
            target = peer(d)
            copy_to(
                target,
                send.at[q, target[3], target[0] * 2 + target[2]],
                recv.at[q, pl.ds(pl.multiple_of(d * CAP, CAP), CAP)],
                row_send.at[q], row_recv.at[q],
            ).start()
            return 0

        lax.fori_loop(1, PLANE, go, 0)

    def rows_of(q):
        rest = recv.at[q, pl.ds(CAP, (PLANE - 1) * CAP)]
        return copy_to(peer(1), rest, rest, row_send.at[q], row_recv.at[q])

    gather(0)
    for copy in small:
        copy.wait()
    pl.semaphore_wait(barrier, PLANE + NZ - 2)

    def send_keys(d, _):
        target = peer(d)
        copy_to(target, key_ref.at[target[0] * 2 + target[2]], keys_in.at[d], key_send, key_recv).start()
        return 0

    start_rows(0)
    lax.fori_loop(1, PLANE, send_keys, 0)
    keys_in[0] = key_ref[mine]
    gather(1)
    start_rows(1)

    heavy_of = lax.broadcasted_iota(jnp.int32, (H, F), 0)

    def heavy_block(b):
        lanes = []
        for i in range(4):
            k = hkey_ref[pl.ds(b * 4 + i, 1), :]
            k = ((k >> 4) & 1) * 512 + ((k >> 5) & 7) * 64 + (k >> 8) * 16 + (k & 15)
            lanes.append(jnp.where(flag_ref[pl.ds(b * 4 + i, 1), :] == 1, k, -1))
        hot = jnp.where(heavy_of == jnp.concatenate(lanes, axis=1), 1.0, 0.0).astype(jnp.bfloat16)
        rows = x_ref[pl.ds(pl.multiple_of(b * 512, 512), 512), :]
        return jnp.dot(hot, rows, preferred_element_type=jnp.float32)

    hacc[...] = heavy_block(0)

    def heavy_step(b, _):
        hacc[...] += heavy_block(b)
        return 0

    lax.fori_loop(1, ROWS // 512, heavy_step, 0)
    halves = H // 2
    half_copy = copy_to(
        twin, hacc.at[pl.ds(pl.multiple_of((1 - c) * halves, halves), halves)], half_in, half_send, half_recv
    )
    half_copy.start()

    all_keys = copy_to(peer(1), keys_in.at[pl.ds(1, PLANE - 1)], keys_in.at[pl.ds(1, PLANE - 1)], key_send, key_recv)

    def pack_keys():
        all_keys.wait_recv()
        lane = lax.broadcasted_iota(jnp.int32, (NZ, LANES), 1)
        for m in range(PLANE // 4):
            k0, k1, k2, k3 = (keys_in[4 * m + i] for i in range(4))
            k1, k2, k3 = pltpu.roll(k1, 96, 1), pltpu.roll(k2, 64, 1), pltpu.roll(k3, 32, 1)
            packed[3 * m] = jnp.where(lane < 96, k0, k1)
            packed[3 * m + 1] = jnp.where(lane < 64, k1, k2)
            packed[3 * m + 2] = jnp.where(lane < 32, k2, k3)

    block = 768
    tiles = block // LANES
    slot_of = lax.broadcasted_iota(jnp.int32, (SLOTS, block), 0)

    def add_up(q):
        plane = (z + FAR_FIRST[q] + NZ) % NZ
        rows_of(q).wait_recv()

        def part(k):
            lanes = jnp.concatenate(
                [packed[k * tiles + i, pl.ds(plane, 1), :] for i in range(tiles)], axis=1
            )
            hot = jnp.where(slot_of == lanes, 1.0, 0.0).astype(jnp.bfloat16)
            rows = recv[q, pl.ds(pl.multiple_of(k * block, block), block), :]
            return jnp.dot(hot, rows, preferred_element_type=jnp.float32)

        acc[q] = part(0)

        def step(k, _):
            acc[q] += part(k)
            return 0

        lax.fori_loop(1, PLANE * CAP // block, step, 0)

    half_of = lax.broadcasted_iota(jnp.int32, (HALF, block), 0)

    def add_up_half(q, start):
        plane = (z + FAR_FIRST[q] + NZ) % NZ
        keys = pl.ds(start, HALF)

        def part(k):
            lanes = jnp.concatenate(
                [packed[k * tiles + i, pl.ds(plane, 1), :] for i in range(tiles)], axis=1
            )
            hot = jnp.where(half_of == lanes - start, 1.0, 0.0).astype(jnp.bfloat16)
            rows = recv[q, pl.ds(pl.multiple_of(k * block, block), block), :]
            return jnp.dot(hot, rows, preferred_element_type=jnp.float32)

        acc[q, keys, :] = part(0) + down_in[-FAR_FIRST[q], keys, :]

        def step(k, _):
            acc[q, keys, :] += part(k)
            return 0

        lax.fori_loop(1, PLANE * CAP // block, step, 0)

    low, high, whole = pl.ds(0, HALF), pl.ds(HALF, HALF), pl.ds(0, SLOTS)

    def up_copy(q, r, part):
        return copy_to(up, acc.at[q, part], up_in.at[r - 1, part], up_send.at[r - 1], up_recv.at[r - 1])

    def down_copy(q, r, part):
        return copy_to(down, acc.at[q, part], down_in.at[r - 1, part], down_send.at[r - 1], down_recv.at[r - 1])

    hlow, hhigh, hwhole = pl.ds(0, 32), pl.ds(32, 32), pl.ds(0, 64)

    def hup_copy(r, part):
        return copy_to(
            up, hrun.at[(z + r) % NZ, part], hup_in.at[r - 1, part], hup_send.at[r - 1], hup_recv.at[r - 1]
        )

    def hdown_copy(r, part):
        return copy_to(
            down, hrun.at[(z + NZ - r) % NZ, part], hdown_in.at[r - 1, part],
            hdown_send.at[r - 1], hdown_recv.at[r - 1],
        )

    def heavy_far():
        half_copy.wait_recv()

        def own(i, _):
            rows = pl.ds(pl.multiple_of(i * 64, 64), 64)
            hrun[i] = hacc[pl.ds(pl.multiple_of(c * halves + i * 64, 64), 64), :] + half_in[rows, :]
            return 0

        lax.fori_loop(0, NZ, own, 0)
        hup_copy(4, hlow).start()
        hdown_copy(4, hhigh).start()

    def heavy_on(r):
        part = hlow if r == 3 else hwhole
        hup_copy(r + 1, part).wait_recv()
        hrun[(z + r) % NZ, part, :] += hup_in[r, part, :]
        hup_copy(r, hwhole).start()
        part = hhigh if r == 3 else hwhole
        hdown_copy(r + 1, part).wait_recv()
        hrun[(z + NZ - r) % NZ, part, :] += hdown_in[r, part, :]
        hdown_copy(r, hwhole).start()

    def part_copy(d):
        target = across(d)
        return copy_to(
            target, hpart.at[target[0] * 4 + target[3]], plane_in.at[d], part_send.at[d], part_recv.at[d]
        )

    def heavy_plane():
        hup_copy(1, hwhole).wait_recv()
        hdown_copy(1, hwhole).wait_recv()
        hrun[z] += hup_in[0] + hdown_in[0]
        for i in range(16):
            hpart[i] = hrun[z, pl.ds(4 * i, 4), :]
        lax.fori_loop(1, 16, lambda d, _: (part_copy(d).start(), 0)[1], 0)

    def line_copy(d):
        return copy_to(
            along(d), hout.at[y, z, c, x], hout.at[y, z, c, x], line_send.at[d], line_recv.at[d]
        )

    def line_from(d):
        spot = hout.at[y, (z + NZ - d) % NZ, c, x]
        return copy_to(along(d), spot, spot, line_send.at[d], line_recv.at[d])

    def heavy_join():
        lax.fori_loop(1, 16, lambda d, _: (part_copy(d).wait_recv(), 0)[1], 0)
        total = hpart[y * 4 + x]
        for d in range(1, 16):
            total += plane_in[d]
        hout[y, z, c, x] = (total * hdims_ref[...].astype(jnp.float32)).astype(jnp.bfloat16)
        lax.fori_loop(1, NZ, lambda d, _: (line_copy(d).start(), 0)[1], 0)

    def sheet_copy(d):
        spot = hout.at[y, :, c, x]
        return copy_to(across(d), spot, spot, sheet_send.at[d], sheet_recv.at[d])

    def sheet_from(d):
        spot = hout.at[(y + 4 - d % 4) % 4, :, c, (x + 4 - d // 4) % 4]
        return copy_to(across(d), spot, spot, sheet_send.at[d], sheet_recv.at[d])

    def heavy_sheet():
        lax.fori_loop(1, NZ, lambda d, _: (line_from(d).wait_recv(), 0)[1], 0)
        lax.fori_loop(1, 16, lambda d, _: (sheet_copy(d).start(), 0)[1], 0)

    def twin_copy(core):
        spot = hout.at[:, :, core]
        return copy_to(twin, spot, spot, twin_send, twin_recv)

    def heavy_twin():
        lax.fori_loop(1, 16, lambda d, _: (sheet_from(d).wait_recv(), 0)[1], 0)
        twin_copy(c).start()

    def lay_out(core):
        def line(i, _):
            spot = hacc.at[pl.ds(pl.multiple_of((i * 2 + core) * 16, 16), 16)]
            for j in range(NX):
                spot[4 * j : 4 * j + 4, :] = hout[i // NZ, i % NZ, core, j].astype(jnp.float32)
            return 0

        lax.fori_loop(0, NY * NZ, line, 0)

    def chain(q):
        r = FAR_FIRST[q]
        if r == 4:
            up_copy(q, 4, low).start()
            down_copy(q, 4, high).start()
        elif r > 0:
            part = low if r == 3 else whole
            up_copy(0, r + 1, part).wait_recv()
            acc[q, part, :] += up_in[r, part, :]
            up_copy(q, r, whole).start()
        elif r < 0:
            part = high if r == -3 else whole
            down_copy(0, 1 - r, part).wait_recv()
            acc[q, part, :] += down_in[-r, part, :]
            down_copy(q, -r, whole).start()
        else:
            up_copy(0, 1, whole).wait_recv()
            down_copy(0, 1, whole).wait_recv()
            total = acc[q] + up_in[0] + down_in[0]
            out_ref[...] = (total * dims_ref[...].astype(jnp.float32)).astype(jnp.bfloat16)

    def issue(q):
        gather(q)
        start_rows(q)

    issue(2)
    heavy_far()
    gather(3)
    heavy_on(3)
    pack_keys()
    add_up(0)
    heavy_on(2)
    start_rows(3)
    add_up(1)
    heavy_on(1)
    chain(0)
    gather(4)
    heavy_plane()
    start_rows(4)
    add_up(2)
    chain(1)
    chain(2)
    gather(5)
    heavy_join()
    start_rows(5)
    add_up(3)
    issue(6)
    add_up(4)
    chain(3)
    chain(4)
    issue(7)
    heavy_sheet()
    add_up(5)
    chain(5)
    down_copy(0, 2, whole).wait_recv()
    rows_of(6).wait_recv()
    for keys in (low, high):
        add_up_half(6, keys.start)
        down_copy(6, 1, keys).start()
    add_up(7)
    heavy_twin()
    half_copy.wait_send()
    lay_out(c)
    chain(7)

    twin_copy(1 - c).wait_recv()
    lay_out(1 - c)
    hfin_ref[...] = hacc[...].astype(jnp.bfloat16)
    twin_copy(c).wait_send()
    lax.fori_loop(1, 16, lambda d, _: (part_copy(d).wait_send(), 0)[1], 0)
    lax.fori_loop(1, 16, lambda d, _: (sheet_copy(d).wait_send(), 0)[1], 0)
    lax.fori_loop(1, NZ, lambda d, _: (line_copy(d).wait_send(), 0)[1], 0)
    all_keys.wait_send()
    for q in range(len(FAR_FIRST)):
        rows_of(q).wait_send()
    for r in range(1, 5):
        up_copy(0, r, low if r == 4 else whole).wait_send()
        down_copy(0, r, high if r == 4 else whole).wait_send()
        hup_copy(r, hlow if r == 4 else hwhole).wait_send()
        hdown_copy(r, hhigh if r == 4 else hwhole).wait_send()


def join(source, key, heavy_key, flag, rows, light_dims, heavy_dims):
    vmem = pl.BlockSpec(memory_space=pltpu.VMEM)
    dma = pltpu.SemaphoreType.DMA
    f32 = jnp.float32
    return pl.pallas_call(
        fused_kernel,
        in_specs=[pl.BlockSpec(memory_space=pltpu.SMEM)]
        + [pl.BlockSpec(memory_space=pl.ANY)] * 6,
        out_specs=(vmem, vmem),
        out_shape=(
            jax.ShapeDtypeStruct((SLOTS, LANES), jnp.bfloat16),
            jax.ShapeDtypeStruct((H, F), jnp.bfloat16),
        ),
        scratch_shapes=[
            pltpu.VMEM((8, NZ, LANES), jnp.int32),
            pltpu.VMEM((ROWS // LANES, LANES), jnp.int32),
            pltpu.VMEM((ROWS // LANES, LANES), jnp.int32),
            pltpu.VMEM((SLOTS, LANES), jnp.bfloat16),
            pltpu.VMEM((4, F), jnp.bfloat16),
            dma((5,)),
            pltpu.VMEM((NY, NZ, NC, NX, 4, F), jnp.bfloat16),
            pltpu.VMEM((ROWS, F), jnp.bfloat16),
            dma((ROWS // X_PART,)),
            pltpu.VMEM((4, ROWS, LANES), f32),
            pltpu.VMEM((4, 8 * CAP, LANES), f32),
            pltpu.VMEM((NZ, NX, 8, CAP, LANES), jnp.bfloat16),
            pltpu.VMEM((NZ, PLANE * CAP, LANES), jnp.bfloat16),
            pltpu.VMEM((PLANE, NZ, LANES), jnp.int32),
            pltpu.VMEM((PLANE * CAP // LANES, NZ, LANES), jnp.int32),
            pltpu.VMEM((4, SLOTS, LANES), f32),
            pltpu.VMEM((4, SLOTS, LANES), f32),
            pltpu.VMEM((NZ, SLOTS, LANES), f32),
            pltpu.VMEM((H, F), f32),
            pltpu.VMEM((H // 2, F), f32),
            pltpu.VMEM((NZ, 64, F), f32),
            pltpu.VMEM((4, 64, F), f32),
            pltpu.VMEM((4, 64, F), f32),
            pltpu.VMEM((16, 4, F), f32),
            pltpu.VMEM((16, 4, F), f32),
            dma, dma, dma((NZ,)), dma((NZ,)), dma((4,)), dma((4,)), dma((4,)), dma((4,)),
            dma, dma, dma((4,)), dma((4,)), dma((4,)), dma((4,)), dma((16,)), dma((16,)),
            dma((NZ,)), dma((NZ,)), dma((16,)), dma((16,)), dma, dma,
        ],
        compiler_params=pltpu.CompilerParams(
            collective_id=0, has_side_effects=True, vmem_limit_bytes=62 << 20
        ),
        name="join",
    )(source, key.reshape(8, NZ, LANES), heavy_key, flag, rows, light_dims, heavy_dims)


def keep_kernel(light_in, heavy_in, light_out, heavy_out, light, heavy, came, gone):
    quarter = H // 4
    spans = [pl.ds(i * quarter, quarter) for i in range(4)]
    moves = [(light_in, light, light_out)] + [
        (heavy_in.at[rows], heavy.at[rows], heavy_out.at[rows]) for rows in spans
    ]
    ins = [pltpu.make_async_copy(a, b, came.at[i]) for i, (a, b, _) in enumerate(moves)]
    outs = [pltpu.make_async_copy(b, c, gone.at[i]) for i, (_, b, c) in enumerate(moves)]
    for copy in ins:
        copy.start()
    for arrives, leaves in zip(ins, outs):
        arrives.wait()
        leaves.start()
    for copy in outs:
        copy.wait()


def keep(light, heavy):
    anywhere = pl.BlockSpec(memory_space=pl.ANY)
    return pl.pallas_call(
        keep_kernel,
        in_specs=[anywhere] * 2,
        out_specs=(anywhere, anywhere),
        out_shape=tuple(jax.ShapeDtypeStruct(v.shape, v.dtype) for v in (light, heavy)),
        scratch_shapes=[
            pltpu.VMEM(light.shape, light.dtype),
            pltpu.VMEM(heavy.shape, heavy.dtype),
            pltpu.SemaphoreType.DMA((5,)),
            pltpu.SemaphoreType.DMA((5,)),
        ],
        name="keep",
    )(light, heavy)


def shards(rows, owner, slot, flag, heavy_key, light_dims, heavy_dims):
    owner, slot, flag, heavy_key = (
        v.reshape(ROWS // LANES, LANES) for v in (owner, slot, flag, heavy_key)
    )
    source, key = tables(owner, slot, flag)
    light_joined, heavy_joined = join(source, key, heavy_key, flag, rows, light_dims, heavy_dims)
    return keep(light_joined, heavy_joined)


def solution(mesh):
    torus = Mesh(mesh.devices.reshape(NY, NZ, NC, NX), ALL)
    rows = P(ALL, None)
    return jax.shard_map(
        shards,
        mesh=torus,
        in_specs=(rows, rows, rows, rows, rows, P(SHUFFLE, "x"), rows),
        out_specs=(P(SHUFFLE, "x"), P()),
        check_vma=False,
    )
```
